32 devices in a mesh: gx: 2 (over x), gy: 16 (over z, y, core).
Axes of the slice: x: 2, y: 2, z: 4, core: 2. Of those that a mesh axis runs over, the one named last changes fastest.
Arguments:
- trial: float32 [49152, 384], P(('gx', 'gy')), may hold values from -30 to 30
- resid: float32 [49152, 128], P(('gx', 'gy')), may hold values from -500 to 500
- energy: float32 [49152], P(('gx', 'gy')), may hold values from 1 to 10
- shift: float32 [128], replicated, may hold values from 0.05 to 0.5
Outputs:
- basis: float32 [49152, 128], P(('gx', 'gy'))
The draws below stay inside these ranges and needn't reach their ends.
All inputs are finite; a program needn't handle non-finite values.
Results may differ from the reference program's by a relative error of at most 0.0003.
Values sent between devices are 32-bit elements; how exact they have to be, the bound alone decides.
A program may use at most 64 MiB of HBM per device.

```python
import math
import jax
import jax.numpy as jnp
from jax import lax

KEEP = 384
NEW = 128
NPAIR = 49152


side_share = 0.01


def base_noise(key, label, height, breadth):
    subkey = jax.random.fold_in(jax.random.fold_in(key, 5101), label)
    return jax.random.truncated_normal(subkey, -5.0, 5.0, (height, breadth), jnp.float32)


def row_scale():
    place = jnp.arange(NPAIR, dtype=jnp.float32) / (NPAIR - 1)
    return jnp.exp(place * math.log(3.0))[:, None]


def energies(key):
    subkey = jax.random.fold_in(jax.random.fold_in(key, 5101), 11)
    level = jax.random.uniform(subkey, (NPAIR,), jnp.float32, 0.0, 1.0)
    return jnp.exp(level * math.log(9.99))


def shifts(key):
    subkey = jax.random.fold_in(jax.random.fold_in(key, 5101), 12)
    return jax.random.uniform(subkey, (NEW,), jnp.float32, 0.05, 0.5)


def draw_trial(key, part):
    return base_noise(key, 1, NPAIR, KEEP) * row_scale()


def draw_energy(key, part):
    return energies(key)


def draw_shift(key, part):
    return shifts(key)


def draw_resid(key, part):
    stored = base_noise(key, 1, NPAIR, KEEP)
    mixkey = jax.random.fold_in(jax.random.fold_in(key, 5101), 2)
    mixing = jax.random.truncated_normal(mixkey, -5.0, 5.0, (KEEP, NEW), jnp.float32) / math.sqrt(KEEP)
    owned = base_noise(key, 5, NPAIR, NEW)
    inside = jnp.dot(stored, mixing, precision=lax.Precision.HIGHEST, preferred_element_type=jnp.float32)
    target = jnp.clip(inside, -7.9, 7.9) + side_share * owned
    target = target * row_scale()
    return target * (energies(key)[:, None] - shifts(key)[None, :])


def setup_inputs(seed: int = 0) -> dict:
    key_list = jax.random.split(jax.random.key(seed), 5)
    return {
        "trial": draw_trial(jax.random.fold_in(key_list[4], 71), 0),
        "resid": draw_resid(jax.random.fold_in(key_list[4], 71), 0),
        "energy": draw_energy(jax.random.fold_in(key_list[4], 71), 0),
        "shift": draw_shift(jax.random.fold_in(key_list[4], 71), 0),
    }


def fdot(left, right):
    return jnp.dot(left.astype(jnp.float32), right.astype(jnp.float32), precision=lax.Precision.HIGHEST, preferred_element_type=jnp.float32)

def reference(trial, resid, energy, shift):
    count = trial.shape[0]
    work = resid / (energy[:, None] - shift[None, :])
    for sweep in range(2):
        coef = fdot(trial.T, work) / count
        work = work - fdot(trial, coef)
    gram = fdot(work.T, work) / count
    lower = jnp.linalg.cholesky(gram)
    return jax.scipy.linalg.solve_triangular(lower, work.T, lower=True).T
```

```python
import functools

import jax
import jax.numpy as jnp
from jax import lax
from jax.experimental import pallas as pl
from jax.experimental.pallas import tpu as pltpu
from jax.sharding import PartitionSpec as P

MESH = pl.DeviceIdType.MESH
LANES = 128
HALF = LANES // 2
ROWS = 256
SHARE_LIMIT = 32.0
LENGTH_LIMIT = 1024.0


def bdot(left, right, dims):
    return lax.dot_general(left, right, (dims, ((), ())), preferred_element_type=jnp.float32)


def chunk_rows(total, owners):
    return -(-total // (8 * owners)) * 8


def ranges(count, step):
    return [(start, min(step, count - start)) for start in range(0, count, step)]


def split(values):
    high = values.astype(jnp.bfloat16)
    rest = values - high.astype(jnp.float32)
    middle = rest.astype(jnp.bfloat16)
    low = (rest - middle.astype(jnp.float32)).astype(jnp.bfloat16)
    return high, middle, low


def dot(left, right, dims):
    return lax.dot_general(
        left, right, (dims, ((), ())),
        precision=lax.Precision.HIGHEST, preferred_element_type=jnp.float32,
    )


def wide(high, middle, low, right):
    a, b, c = split(right)
    both = jnp.concatenate([a, b], axis=1)
    width = right.shape[1]
    one = bdot(high, both, ((1,), (0,)))
    two = bdot(middle, both, ((1,), (0,)))
    rest = bdot(high, c, ((1,), (0,))) + bdot(low, a, ((1,), (0,)))
    return one[:, :width] + (one[:, width:] + two[:, :width] + (rest + two[:, width:]))


def outer(left, right):
    a, b, c = split(left)
    d, e, f = split(right)
    return lax.dot_general(
        jnp.concatenate([a, a, b, b, a, c], 0), jnp.concatenate([d, e, d, e, f, d], 0),
        (((0,), (0,)), ((), ())), preferred_element_type=jnp.float32)


def inverse_factor(square, width):
    size = square.shape[0]
    row = lax.broadcasted_iota(jnp.int32, (size, size), 0)
    col = lax.broadcasted_iota(jnp.int32, (size, size), 1)
    both = jnp.concatenate([square, (row == col).astype(jnp.float32)], axis=1)
    local = lax.broadcasted_iota(jnp.int32, (width, size), 0)
    out, scales = [], []
    for start in range(0, size, width):
        slab, side = both[:width, :size], both[:width, size:]
        cols = [jnp.broadcast_to(slab[:, start + j:start + j + 1], (width, size)) for j in range(width)]
        scale = jnp.ones((width, size), jnp.float32)
        for j in range(width):
            inverse = 1.0 / cols[j][j:j + 1, :]
            factor = jnp.where(local > j, cols[j] * inverse, 0.0)
            scale = jnp.where(local == j, inverse, scale)
            for m in range(j + 1, width):
                cols[m] = cols[m] - factor * cols[m][j:j + 1, :]
            slab = slab - factor * slab[j:j + 1, :]
            side = side - factor * side[j:j + 1, :]
        out.append(side * jnp.sqrt(scale))
        scales.append(scale)
        if start + width < size:
            update = outer(slab * scale, jnp.concatenate([slab, side], axis=1))
            both = both[width:] - update[start + width:]
    return jnp.concatenate(out, axis=0), jnp.concatenate(scales, axis=0)


def robust_kernel(
    nx, ny, count, trial, resid, energy, shift, basis,
    xs, xh, xm, xl, wh, wm, wl, held, load, load_resid, gram, part, swap, acc, landed, red, full, gpart, glanded, gred,
    swap_send, swap_recv, rs_send, rs_recv, ag_send, ag_recv, fw_send, fw_recv,
    gs_send, gs_recv, ga_send, ga_recv,
):
    ix, iy = lax.axis_index("gx"), lax.axis_index("gy")
    pairs_y = ny // 2
    np_ = nx * pairs_y
    ndev = nx * ny
    me, core = ix * pairs_y + iy // 2, iy % 2
    flat = me * 2 + core
    kept = trial.shape[1]
    keep = kept // LANES
    fetch = pltpu.make_async_copy(trial, xs.at[:, pl.ds(0, kept)], load)
    fetch.start()
    fetch_resid = pltpu.make_async_copy(resid, held, load_resid)
    fetch_resid.start()
    rows = trial.shape[0]
    half = acc.shape[0]
    rs_rows = red.shape[0]
    owners = half // rs_rows
    g_rows = gred.shape[0]
    g_owners = LANES // g_rows

    def where(pair, which):
        return (pair // pairs_y, (pair % pairs_y) * 2 + which)

    def others(total, mine, body):
        def step(k, carry):
            body(lax.rem(mine + k, total))
            return carry
        lax.fori_loop(1, total, step, 0)

    barrier = pltpu.get_barrier_semaphore()

    def greet(other):
        pl.semaphore_signal(barrier, inc=1, device_id=where(other // 2, other % 2), device_id_type=MESH)
    others(ndev, flat, greet)

    fetch_resid.wait()
    for block in range(rows // LANES):
        span = pl.ds(block * LANES, LANES)
        level = jnp.broadcast_to(energy[block:block + 1, :], (LANES, LANES)).T
        xs[span, kept:] = held[span, :] / (level - shift[...])
    fetch.wait()
    for start, size in ranges(rows, LANES):
        span = pl.ds(start, size)
        xh[span, :], xm[span, :], xl[span, :] = split(xs[span, :])

    slots = {}
    spans = []
    for i in range(keep):
        first_place = len(slots)
        for j in range(i, keep):
            slots[i, j] = len(slots)
        slots["r", i] = len(slots)
        spans.append((first_place * HALF, len(slots) * HALF))

    def stripe(i):
        left, right = pl.ds(i * LANES, LANES), slice(i * LANES, None)
        total = None
        for one, two in ((xm, xm), (xl, xh), (xh, xl), (xm, xh), (xh, xm), (xh, xh)):
            term = bdot(one[:, left], two[:, right], ((0,), (0,)))
            total = term if total is None else total + term
        for j in range(keep - i + 1):
            start = spans[i][0] + j * HALF
            for which in range(2):
                part[pl.ds(which * half + start, HALF), :] = total[
                    which * HALF:(which + 1) * HALF, j * LANES:(j + 1) * LANES]

    def read(name):
        return jnp.concatenate(
            [full[pl.ds(which * half + slots[name] * HALF, HALF), :] for which in range(2)], axis=0)

    def rows_of(index, size, base=0):
        return pl.ds(pl.multiple_of(base + index * size, 8), size)

    def exchange(i):
        low, high = spans[i]
        return pltpu.make_async_remote_copy(
            src_ref=part.at[pl.ds(pl.multiple_of((1 - core) * half + low, 8), high - low)],
            dst_ref=swap.at[pl.ds(low, high - low)],
            send_sem=swap_send.at[i], recv_sem=swap_recv.at[i],
            device_id=where(me, 1 - core), device_id_type=MESH)

    def scatter(other):
        return pltpu.make_async_remote_copy(
            src_ref=acc.at[rows_of(other, rs_rows)], dst_ref=landed.at[me],
            send_sem=rs_send.at[other], recv_sem=rs_recv.at[me],
            device_id=where(other, core), device_id_type=MESH)

    def scatter_in(other):
        return pltpu.make_async_remote_copy(
            src_ref=acc.at[rows_of(0, rs_rows)], dst_ref=landed.at[other],
            send_sem=rs_send.at[other], recv_sem=rs_recv.at[other],
            device_id=where(other, core), device_id_type=MESH)

    def guarded(limit, body):
        def run(other):
            if limit >= np_:
                body(other)
            else:
                @pl.when(other < limit)
                def _():
                    body(other)
        return run

    sent = [0]

    def absorb(i):
        low, high = spans[i]
        exchange(i).wait_recv()
        acc[pl.ds(low, high - low), :] = (
            part[pl.ds(pl.multiple_of(core * half + low, 8), high - low), :] + swap[pl.ds(low, high - low), :])
        begin, end = sent[0], owners if i == keep - 1 else high // rs_rows
        sent[0] = end

        def send(k, carry):
            other = begin + lax.rem(me + k, end - begin)

            @pl.when(other != me)
            def _():
                scatter(other).start()
            return carry
        lax.fori_loop(0, end - begin, send, 0)

    if spans[-1][1] < half:
        acc[pl.ds(spans[-1][1], half - spans[-1][1]), :] = jnp.zeros((half - spans[-1][1], LANES), jnp.float32)
    for i in range(keep):
        stripe(i)
        if i == 0:
            pl.semaphore_wait(barrier, ndev - 1)
        exchange(i).start()
        if i > 0:
            absorb(i - 1)
    absorb(keep - 1)

    base = core * half

    def gather(other):
        return pltpu.make_async_remote_copy(
            src_ref=red, dst_ref=full.at[rows_of(me, rs_rows, base)],
            send_sem=ag_send.at[other], recv_sem=ag_recv.at[me],
            device_id=where(other, core), device_id_type=MESH)

    def gather_in(other):
        return pltpu.make_async_remote_copy(
            src_ref=red, dst_ref=full.at[rows_of(other, rs_rows, base)],
            send_sem=ag_send.at[other], recv_sem=ag_recv.at[other],
            device_id=where(other, core), device_id_type=MESH)

    def forward(owner, source):
        return pltpu.make_async_remote_copy(
            src_ref=source, dst_ref=full.at[rows_of(owner, rs_rows, base)],
            send_sem=fw_send.at[owner], recv_sem=fw_recv.at[owner],
            device_id=where(me, 1 - core), device_id_type=MESH)

    def forward_in(owner):
        return pltpu.make_async_remote_copy(
            src_ref=red, dst_ref=full.at[rows_of(owner, rs_rows, half - base)],
            send_sem=fw_send.at[owner], recv_sem=fw_recv.at[owner],
            device_id=where(me, 1 - core), device_id_type=MESH)

    @pl.when(me < owners)
    def _():
        others(np_, me, lambda other: scatter_in(other).wait_recv())
        landed[me] = acc[rows_of(me, rs_rows), :]
        red[...] = lax.fori_loop(0, np_, lambda k, total: total + landed[k], jnp.zeros(red.shape, jnp.float32))
        others(np_, me, lambda other: gather(other).start())
        forward(me, red).start()
        full[rows_of(me, rs_rows, base), :] = red[...]

    def relay(other):
        gather_in(other).wait_recv()
        forward(other, full.at[rows_of(other, rs_rows, base)]).start()
    others(np_, me, guarded(owners, relay))
    lax.fori_loop(0, owners, lambda k, carry: (forward_in(k).wait_recv(), carry)[1], 0)

    raw = [read(("r", i)) for i in range(keep)]
    first = [one / count for one in raw]
    total = []
    for i in range(keep):
        metric = None
        for j in range(keep):
            block = read((min(i, j), max(i, j)))
            term = dot(block, first[j], ((1,), (0,)) if i <= j else ((0,), (0,)))
            metric = term if metric is None else metric + term
        total.append(first[i] + (raw[i] - metric) / count)
    coef = jnp.concatenate(total, axis=0)
    for start, size in ranges(rows, 256):
        span = pl.ds(start, size)
        block = xs[span, kept:] - wide(xh[span, :kept], xm[span, :kept], xl[span, :kept], coef)
        wh[span, :], wm[span, :], wl[span, :] = split(block)
    ours = wh[...]
    high = bdot(ours, ours, ((0,), (0,)))
    cross = bdot(ours, wm[...], ((0,), (0,))) + bdot(ours, wl[...], ((0,), (0,)))
    gpart[...] = high + (cross + cross.T + bdot(wm[...], wm[...], ((0,), (0,))))

    def gscatter(other):
        return pltpu.make_async_remote_copy(
            src_ref=gpart.at[rows_of(other, g_rows)], dst_ref=glanded.at[flat],
            send_sem=gs_send.at[other], recv_sem=gs_recv.at[flat],
            device_id=where(other, 0), device_id_type=MESH)

    def gscatter_in(other):
        return pltpu.make_async_remote_copy(
            src_ref=gpart.at[rows_of(0, g_rows)], dst_ref=glanded.at[other],
            send_sem=gs_send.at[0], recv_sem=gs_recv.at[other],
            device_id=where(other // 2, other % 2), device_id_type=MESH)

    def ggather(other):
        return pltpu.make_async_remote_copy(
            src_ref=gred, dst_ref=gram.at[rows_of(me, g_rows)],
            send_sem=ga_send.at[other], recv_sem=ga_recv.at[me],
            device_id=where(other // 2, other % 2), device_id_type=MESH)

    def ggather_in(owner):
        return pltpu.make_async_remote_copy(
            src_ref=gred, dst_ref=gram.at[rows_of(owner, g_rows)],
            send_sem=ga_send.at[0], recv_sem=ga_recv.at[owner],
            device_id=where(owner, 0), device_id_type=MESH)

    others(np_, me, guarded(g_owners, lambda other: gscatter(other).start()))

    @pl.when(jnp.logical_and(core == 1, me < g_owners))
    def _():
        gscatter(me).start()

    for i in range(keep):
        exchange(i).wait_send()
    others(np_, me, guarded(owners, lambda other: scatter(other).wait_send()))

    @pl.when(me < owners)
    def _():
        others(np_, me, lambda other: gather(other).wait_send())
    lax.fori_loop(0, owners, lambda k, carry: (forward_in(k).wait_send(), carry)[1], 0)
    others(np_, me, guarded(g_owners, lambda other: gscatter(other).wait_send()))

    @pl.when(jnp.logical_and(core == 1, me < g_owners))
    def _():
        gscatter(me).wait_send()

    @pl.when(jnp.logical_and(core == 0, me < g_owners))
    def _():
        others(ndev, flat, lambda other: gscatter_in(other).wait_recv())
        glanded[flat] = gpart[rows_of(me, g_rows), :]
        gred[...] = lax.fori_loop(
            0, ndev, lambda k, total: total + glanded[k], jnp.zeros(gred.shape, jnp.float32)) / count
        others(ndev, flat, lambda other: ggather(other).start())
        gram[rows_of(me, g_rows), :] = gred[...]

    others(np_, me, guarded(g_owners, lambda other: ggather_in(other).wait_recv()))

    @pl.when(jnp.logical_and(core == 1, me < g_owners))
    def _():
        ggather_in(me).wait_recv()

    inverse = inverse_factor(gram[...], 16)[0].T
    for start, size in ranges(rows, 256):
        span = pl.ds(start, size)
        basis[span, :] = wide(wh[span, :], wm[span, :], wl[span, :], inverse)

    @pl.when(jnp.logical_and(core == 0, me < g_owners))
    def _():
        others(ndev, flat, lambda other: ggather(other).wait_send())


def robust_call(nx, ny, trial, resid, energy, shift):
    rows, kept = trial.shape
    new = resid.shape[1]
    keep = kept // LANES
    blocks = keep + keep * (keep + 1) // 2
    np_ = nx * (ny // 2)
    rs_rows = chunk_rows(blocks * HALF, np_)
    owners = -(-blocks * HALF // rs_rows)
    half = owners * rs_rows
    g_rows = chunk_rows(LANES, np_)
    f32 = jnp.float32
    dma = pltpu.SemaphoreType.DMA
    vmem = pl.BlockSpec(memory_space=pltpu.VMEM)
    return pl.pallas_call(
        functools.partial(robust_kernel, nx, ny, float(rows * nx * ny)),
        name="robust",
        out_shape=jax.ShapeDtypeStruct((rows, new), f32),
        in_specs=[pl.BlockSpec(memory_space=pl.ANY)] * 2 + [vmem] * 2,
        out_specs=vmem,
        scratch_shapes=[
            pltpu.VMEM((rows, kept + new), f32),
            *[pltpu.VMEM((rows, kept + new), jnp.bfloat16)] * 3,
            *[pltpu.VMEM((rows, new), jnp.bfloat16)] * 3,
            pltpu.VMEM((rows, new), f32),
            dma, dma,
            pltpu.VMEM((new, new), f32),
            pltpu.VMEM((2 * half, LANES), f32),
            pltpu.VMEM((half, LANES), f32),
            pltpu.VMEM((half, LANES), f32),
            pltpu.VMEM((np_, rs_rows, LANES), f32),
            pltpu.VMEM((rs_rows, LANES), f32),
            pltpu.VMEM((2 * half, LANES), f32),
            pltpu.VMEM((LANES, LANES), f32),
            pltpu.VMEM((nx * ny, g_rows, LANES), f32),
            pltpu.VMEM((g_rows, LANES), f32),
            dma((keep,)), dma((keep,)), dma((np_,)), dma((np_,)), dma((np_,)), dma((np_,)), dma((owners,)), dma((owners,)),
            dma((np_,)), dma((nx * ny,)), dma((nx * ny,)), dma((np_,)),
        ],
        compiler_params=pltpu.CompilerParams(collective_id=1, has_side_effects=True),
    )(trial, resid, energy, shift)


def halves(values):
    high = values.astype(jnp.bfloat16)
    return high, (values - high.astype(jnp.float32)).astype(jnp.bfloat16)


def dot3(left, right):
    a, b = left
    c, d = right
    width = c.shape[1]
    one = bdot(a, jnp.concatenate([c, d], axis=1), ((1,), (0,)))
    return one[:, :width] + (one[:, width:] + bdot(b, c, ((1,), (0,))))


def plan(kept, new, owners):
    blocks = (kept + new) // LANES
    names, late = [], []
    for i in range(0, blocks, 2):
        pair = [(i, i)] + ([(i + 1, i + 1)] if i + 1 < blocks else [])
        (names if i == 0 else late).append(("pack", *[p[0] for p in pair]))
    for i in range(blocks):
        for j in range(i + 1, blocks):
            (names if i == 0 else late).append((i, j))
    parts = []
    start = 0
    for group in (names, late):
        rows = -(-len(group) * HALF // (8 * owners)) * 8 * owners
        parts.append((group, start, rows))
        start += rows
    return parts, start, start + 8


def reduce_kernel(
    nx, ny, count, trial, resid, energy, shift, high_out, low_out, last_out, safe,
    xs, xh, xm, held, load, load_resid, part, swap, acc, landed, landed_tail, red, red_tail, full,
    swap_send, swap_recv, rs_send, rs_recv, ag_send, ag_recv, fw_send, fw_recv,
):
    ix, iy = lax.axis_index("gx"), lax.axis_index("gy")
    pairs_y = ny // 2
    np_ = nx * pairs_y
    ndev = nx * ny
    me, core = ix * pairs_y + iy // 2, iy % 2
    flat = me * 2 + core
    rows, kept = trial.shape
    new = resid.shape[1]
    keep = kept // LANES
    blocks = keep + 1
    groups, tail, half = plan(kept, new, np_)
    center = np_ // 4
    fetch_resid = pltpu.make_async_copy(resid, held, load_resid)
    fetch_resid.start()
    fetch = pltpu.make_async_copy(trial, xs, load)
    fetch.start()

    def where(pair, which):
        return (pair // pairs_y, (pair % pairs_y) * 2 + which)

    def others(total, mine, body):
        def step(k, carry):
            body(lax.rem(mine + 1 + lax.rem(k + total // 4, total - 1), total))
            return carry
        lax.fori_loop(0, total - 1, step, 0)

    barrier = pltpu.get_barrier_semaphore()

    def greet(other):
        pl.semaphore_signal(barrier, inc=1, device_id=where(other // 2, other % 2), device_id_type=MESH)
    others(ndev, flat, greet)

    with jax.named_scope("corr"):
        fetch_resid.wait()
        for block in range(rows // LANES):
            span = pl.ds(block * LANES, LANES)
            level = jnp.broadcast_to(energy[block:block + 1, :], (LANES, LANES)).T
            corr = held[span, :] / (level - shift[...])
            held[span, :] = corr
            xh[span, kept:], xm[span, kept:] = halves(corr)
    with jax.named_scope("fetchsplit"):
        fetch.wait()
        for start, size in ranges(rows, LANES):
            span = pl.ds(start, size)
            xh[span, :kept], xm[span, :kept] = halves(xs[span, :])

    row = lax.broadcasted_iota(jnp.int32, (LANES, LANES), 0)
    col = lax.broadcasted_iota(jnp.int32, (LANES, LANES), 1)

    def save(start, value):
        size = value.shape[0] // 2
        for which in range(2):
            part[pl.ds(which * half + start, size), :] = value[which * size:(which + 1) * size, :]

    found = {}

    def stage(i):
        left, right = pl.ds(i * LANES, min(2, blocks - i) * LANES), slice(i * LANES, None)
        total = None
        for one, two in ((xm, xh), (xh, xm), (xh, xh)):
            term = bdot(one[:, left], two[:, right], ((0,), (0,)))
            total = term if total is None else total + term
        for a in range(i, min(i + 2, blocks)):
            for b in range(a, blocks):
                found[a, b] = total[(a - i) * LANES:(a - i + 1) * LANES, (b - i) * LANES:(b - i + 1) * LANES]

    def store(g):
        names, start, size = groups[g]
        for k, name in enumerate(names):
            if name[0] != "pack":
                value = found[name]
            elif len(name) == 2:
                value = found[name[1], name[1]]
            else:
                value = jnp.where(row <= col, found[name[1], name[1]], found[name[2], name[2]])
            save(start + k * HALF, value)
        if size > len(names) * HALF:
            spare = size - len(names) * HALF
            save(start + len(names) * HALF, jnp.zeros((2 * spare, LANES), jnp.float32))

    def parcel(g):
        if g < len(groups):
            return groups[g][1], groups[g][2]
        return tail, half - tail

    def exchange(g):
        low, size = parcel(g)
        if g == len(groups) - 1:
            size = half - low
        return pltpu.make_async_remote_copy(
            src_ref=part.at[pl.ds(pl.multiple_of((1 - core) * half + low, 8), size)],
            dst_ref=swap.at[pl.ds(low, size)],
            send_sem=swap_send.at[g], recv_sem=swap_recv.at[g],
            device_id=where(me, 1 - core), device_id_type=MESH)

    def absorb(g):
        low, size = parcel(g)
        if g == len(groups) - 1:
            size = half - low
        exchange(g).wait_recv()
        acc[pl.ds(low, size), :] = (
            part[pl.ds(pl.multiple_of(core * half + low, 8), size), :] + swap[pl.ds(low, size), :])

    def each(g):
        return parcel(g)[1] // np_ if g < len(groups) else half - tail

    def spot(g, owner, base=0):
        if g == len(groups):
            return pl.ds(pl.multiple_of(base + tail, 8), each(g))
        return pl.ds(pl.multiple_of(base + groups[g][1] + owner * each(g), 8), each(g))

    def inbox(g):
        return landed_tail if g == len(groups) else landed.at[g, :, pl.ds(0, each(g))]

    def outbox(g):
        return red_tail if g == len(groups) else red.at[g, pl.ds(0, each(g))]

    def scatter(g, other):
        return pltpu.make_async_remote_copy(
            src_ref=acc.at[spot(g, other)], dst_ref=inbox(g).at[me],
            send_sem=rs_send.at[g], recv_sem=rs_recv.at[g],
            device_id=where(other, core), device_id_type=MESH)

    def scatter_all(g):
        others(np_, me, lambda other: scatter(g, other).start())

    def scatter_wait(g, way):
        copy = pltpu.make_async_remote_copy(
            src_ref=inbox(g).at[pl.ds(0, np_ - 1)], dst_ref=inbox(g).at[pl.ds(0, np_ - 1)],
            send_sem=rs_send.at[g], recv_sem=rs_recv.at[g],
            device_id=where(me, core), device_id_type=MESH)
        getattr(copy, way)()

    base = core * half

    def gather(g, other):
        return pltpu.make_async_remote_copy(
            src_ref=outbox(g), dst_ref=full.at[spot(g, me, base)],
            send_sem=ag_send.at[g], recv_sem=ag_recv.at[g],
            device_id=where(other, core), device_id_type=MESH)

    def gather_wait(g, way):
        copy = pltpu.make_async_remote_copy(
            src_ref=inbox(g).at[pl.ds(0, np_ - 1)], dst_ref=inbox(g).at[pl.ds(0, np_ - 1)],
            send_sem=ag_send.at[g], recv_sem=ag_recv.at[g],
            device_id=where(me, core), device_id_type=MESH)
        getattr(copy, way)()

    def forward(g, origin):
        low, size = parcel(g)
        return pltpu.make_async_remote_copy(
            src_ref=full.at[pl.ds(pl.multiple_of(origin + low, 8), size)],
            dst_ref=full.at[pl.ds(pl.multiple_of(origin + low, 8), size)],
            send_sem=fw_send.at[g], recv_sem=fw_recv.at[g],
            device_id=where(me, 1 - core), device_id_type=MESH)

    def total_of(g):
        inbox(g)[me] = acc[spot(g, me), :]
        outbox(g)[...] = lax.fori_loop(
            1, np_, lambda k, total: total + inbox(g)[k], inbox(g)[0])
        full[spot(g, me, base), :] = outbox(g)[...]

    with jax.named_scope("stage0"):
        stage(0)
        store(0)
    with jax.named_scope("bar"):
        pl.semaphore_wait(barrier, ndev - 1)
    exchange(0).start()
    with jax.named_scope("stage1"):
        for i in range(2, blocks, 2):
            stage(i)
        store(1)
        extra = [jnp.sum(jnp.where(row == col, found[i, i], 0.0), axis=0, keepdims=True) for i in range(1, blocks, 2)]
        extra.append(jnp.zeros((16 - len(extra), LANES), jnp.float32))
        save(tail, jnp.concatenate(extra, axis=0))
    exchange(1).start()
    with jax.named_scope("absorb"):
        absorb(0)
        scatter_all(0)
        absorb(1)
        scatter_all(1)
        @pl.when(me != center)
        def _():
            scatter(2, center).start()
    for g in range(2):
        with jax.named_scope(f"rs{g}"):
            scatter_wait(g, "wait_recv")
            total_of(g)
            others(np_, me, lambda other: gather(g, other).start())

    with jax.named_scope("rs2"):
        @pl.when(me == center)
        def _():
            scatter_wait(2, "wait_recv")
            total_of(2)
            others(np_, me, lambda other: gather(2, other).start())
    with jax.named_scope("ag0"):
        gather_wait(0, "wait_recv")
        forward(0, base).start()
    with jax.named_scope("ag1"):
        gather_wait(1, "wait_recv")
        forward(1, base).start()
    with jax.named_scope("ag2"):
        @pl.when(me != center)
        def _():
            gather(2, me).wait_recv()
        forward(2, base).start()
    with jax.named_scope("drain"):
        for g in range(2):
            exchange(g).wait_send()
            scatter_wait(g, "wait_send")
            gather_wait(g, "wait_send")

        @pl.when(me != center)
        def _():
            scatter(2, center).wait_send()

        @pl.when(me == center)
        def _():
            gather_wait(2, "wait_send")
    with jax.named_scope("fw"):
        for g in range(3):
            forward(g, half - base).wait_recv()

    def block_at(start):
        return jnp.concatenate([full[pl.ds(which * half + start, HALF), :] for which in range(2)], axis=0)

    with jax.named_scope("coef"):
        ends = jnp.concatenate([full[pl.ds(which * half + tail, 8), :] for which in range(2)], axis=0)
        value = {}
        for names, start, _ in groups:
            for k, name in enumerate(names):
                block = block_at(start + k * HALF) / count
                if name[0] != "pack":
                    value[name] = block
                elif len(name) == 2:
                    value[name[1], name[1]] = block
                else:
                    place = name[2] // 2
                    flip = block.T
                    value[name[1], name[1]] = jnp.where(row <= col, block, flip)
                    diagonal = jnp.broadcast_to(ends[place:place + 1, :] / count, (LANES, LANES))
                    value[name[2], name[2]] = jnp.where(row == col, diagonal, jnp.where(row > col, block, flip))
        metric = jnp.concatenate([
            jnp.concatenate([value[i, j] if i <= j else value[j, i].T for j in range(keep)], axis=1)
            for i in range(keep)], axis=0)
        first = jnp.concatenate([value[i, keep] for i in range(keep)], axis=0)
        own = value[keep, keep]
        split_metric = halves(metric)
        once = dot3(split_metric, halves(first))
        coef = first + (first - once)
        split_coef = halves(coef)
        twice = dot3(split_metric, split_coef)
        rest = first + (first - twice)
    with jax.named_scope("gramalg"):
        a, b = split_coef
        c, d = halves(rest)
        one = bdot(a, jnp.concatenate([c, d], axis=1), ((0,), (0,)))
        cross = one[:, :LANES] + (one[:, LANES:] + bdot(b, c, ((0,), (0,))))
        gram = own - 0.5 * (cross + cross.T)
    with jax.named_scope("guard"):
        norm = jnp.sum(jnp.abs(metric), axis=0, keepdims=True)
        norm = jnp.max(norm, axis=1, keepdims=True)
        share = jnp.sum(jnp.where(row == col, own, 0.0), axis=0, keepdims=True) + jnp.sum(
            jnp.abs(coef) * (2.0 * jnp.abs(first) + jnp.abs(twice)), axis=0, keepdims=True)
        lengths = jnp.sum(first * first, axis=0, keepdims=True)
        need = jnp.maximum(share * (1.0 / SHARE_LIMIT), norm * (2.0 + norm) * (2.0 + norm) * lengths * (1.0 / LENGTH_LIMIT))
    with jax.named_scope("work"):
        for start, size in ranges(rows, ROWS):
            span = pl.ds(start, size)
            work = held[span, :] - dot3((xh[span, :kept], xm[span, :kept]), split_coef)
            high_out[span, :], low_out[span, :] = halves(work)
    with jax.named_scope("factor"):
        inverse, scales = inverse_factor(gram, 16)
        last_out[...] = inverse.T
        fine = jnp.logical_and(scales > 0.0, need * scales < 1.0)
        good = jnp.where(jnp.logical_and(row == col, jnp.logical_not(fine)), 0.0, 1.0)
        safe[0, 0] = jnp.min(good).astype(jnp.int32)
    with jax.named_scope("drain2"):
        for g in range(3):
            forward(g, base).wait_send()


def reduce_call(nx, ny, trial, resid, energy, shift):
    rows, kept = trial.shape
    new = resid.shape[1]
    np_ = nx * (ny // 2)
    groups, tail, half = plan(kept, new, np_)
    most = max(size // np_ for _, _, size in groups)
    f32, bf16 = jnp.float32, jnp.bfloat16
    dma = pltpu.SemaphoreType.DMA
    vmem = pl.BlockSpec(memory_space=pltpu.VMEM)
    return pl.pallas_call(
        functools.partial(reduce_kernel, nx, ny, float(rows * nx * ny)),
        name="reduce",
        out_shape=(
            jax.ShapeDtypeStruct((rows, new), bf16), jax.ShapeDtypeStruct((rows, new), bf16),
            jax.ShapeDtypeStruct((new, new), f32), jax.ShapeDtypeStruct((1, 1), jnp.int32)),
        in_specs=[pl.BlockSpec(memory_space=pl.ANY)] * 2 + [vmem] * 2,
        out_specs=(vmem, vmem, vmem, pl.BlockSpec(memory_space=pltpu.SMEM)),
        scratch_shapes=[
            pltpu.VMEM((rows, kept), f32),
            *[pltpu.VMEM((rows, kept + new), bf16)] * 2,
            pltpu.VMEM((rows, new), f32),
            dma, dma,
            pltpu.VMEM((2 * half, LANES), f32),
            pltpu.VMEM((half, LANES), f32),
            pltpu.VMEM((half, LANES), f32),
            pltpu.VMEM((2, np_, most, LANES), f32),
            pltpu.VMEM((np_, half - tail, LANES), f32),
            pltpu.VMEM((2, most, LANES), f32),
            pltpu.VMEM((half - tail, LANES), f32),
            pltpu.VMEM((2 * half, LANES), f32),
            dma((2,)), dma((2,)), dma((3,)), dma((3,)), dma((3,)), dma((3,)), dma((3,)), dma((3,)),
        ],
        compiler_params=pltpu.CompilerParams(collective_id=0, has_side_effects=True),
    )(trial, resid, energy, shift)


def apply_kernel(high, low, last, basis, out, store):
    rows = high.shape[0]
    pieces = ranges(rows, 2 * ROWS)

    def put(k):
        start, size = pieces[k]
        return pltpu.make_async_copy(out.at[pl.ds(start, size)], basis.at[pl.ds(start, size)], store.at[k])

    right = halves(last[...])
    for k, (start, size) in enumerate(pieces):
        span = pl.ds(start, size)
        out[span, :] = dot3((high[span, :], low[span, :]), right)
        put(k).start()
    for k in range(len(pieces)):
        put(k).wait()


def apply_call(high, low, last):
    rows, new = high.shape
    dma = pltpu.SemaphoreType.DMA
    vmem = pl.BlockSpec(memory_space=pltpu.VMEM)
    return pl.pallas_call(
        apply_kernel,
        name="apply",
        out_shape=jax.ShapeDtypeStruct((rows, new), jnp.float32),
        in_specs=[vmem, vmem, vmem],
        out_specs=pl.BlockSpec(memory_space=pl.ANY),
        scratch_shapes=[pltpu.VMEM((rows, new), jnp.float32), dma((len(ranges(rows, 2 * ROWS)),))],
    )(high, low, last)


def hand_on(values):
    def body(source, target):
        target[...] = source[...]
    return pl.pallas_call(body, name="hand_on", out_shape=jax.ShapeDtypeStruct(values.shape, values.dtype))(values)


def per_device(nx, ny, trial, resid, energy, shift):
    rows, new = resid.shape
    energy = energy.reshape(rows // LANES, LANES)
    shift = shift.reshape(1, new)
    high, low, last, safe = reduce_call(nx, ny, trial, resid, energy, shift)
    return lax.cond(
        safe[0, 0] > 0,
        lambda: apply_call(high, low, last),
        lambda: hand_on(robust_call(nx, ny, trial, resid, energy, shift)))


def solution(mesh):
    in_specs = (P(("gx", "gy"), None), P(("gx", "gy"), None), P(("gx", "gy")), P())
    out_specs = P(("gx", "gy"), None)
    body = functools.partial(per_device, mesh.shape["gx"], mesh.shape["gy"])
    return jax.shard_map(body, mesh=mesh, in_specs=in_specs, out_specs=out_specs, check_vma=False)
```
